32 devices in a mesh: pipe: 2 (over x), dp: 4 (over z), tensor: 4 (over y, core).
Axes of the slice: x: 2, y: 2, z: 4, core: 2. Of those that a mesh axis runs over, the one named last changes fastest.
Arguments:
- acts_in: bfloat16 [2, 512, 4096], P(None, 'dp', 'tensor'), may hold values from -6 to 6
- weights: bfloat16 [2, 4096, 4096], P('pipe', None, 'tensor'), may hold values from -0.046875 to 0.046875
- cotangent: bfloat16 [2, 512, 4096], P(None, 'dp', 'tensor'), may hold values from -6 to 6
- hist_act: float32 [2, 16], P('pipe'), may hold values from 2 to 12
- hist_weight: float32 [2, 16], P('pipe'), may hold values from 0.01 to 0.1
- hist_grad: float32 [2, 16], P('pipe'), may hold values from 2 to 12
Outputs:
- section_acts: bfloat16 [2, 2, 512, 4096], P('pipe', None, 'dp', 'tensor')
- section_grads: bfloat16 [2, 2, 512, 4096], P('pipe', None, 'dp', 'tensor')
- weight_grad: bfloat16 [2, 4096, 4096], P('pipe', 'dp', 'tensor')
- new_hist_act: float32 [2, 16], P('pipe')
- new_hist_weight: float32 [2, 16], P('pipe')
- new_hist_grad: float32 [2, 16], P('pipe')
The draws below stay inside these ranges and needn't reach their ends.
All inputs are finite; a program needn't handle non-finite values.
Results may differ from the reference program's by a relative error of at most 0.025.
Values may be sent and summed in bfloat16 or wider, within the bound.
A program may use at most 128 MiB of HBM per device.

```python
import math
import jax
import jax.numpy as jnp
from jax import lax

D = 4096
ROWS = 128
MICRO = 2
HIST = 16
SECTIONS = 2
BATCH = 512
N_DP = 4
N_TENSOR = 4


def steps_of(key, dims, split, least, high):
    factor_of, own = 1.0, jax.random.fold_in(key, 6)
    for axis_at, blocks in split:
        draws = jnp.exp(jax.random.uniform(jax.random.fold_in(own, axis_at), (blocks,), jnp.float32, least / len(split), high / len(split)))
        factor_of = factor_of * jnp.repeat(draws, dims[axis_at] // blocks).reshape([-1 if axis == axis_at else 1 for axis in range(len(dims))])
    return factor_of


def centred(rng, shape, scale, reach, pieces=(), kind=jnp.bfloat16):
    factor_of = steps_of(rng, shape, pieces, -0.22, 0.18) if pieces else 1.0
    result = jax.random.normal(rng, shape, jnp.float32) * scale * factor_of
    return jnp.minimum(jnp.maximum(result, -reach), reach).astype(kind)


def setup_inputs(seed: int = 0) -> dict:
    seeds = jax.random.split(jax.random.key(seed), 7)
    acts_in = centred(seeds[0], (MICRO, BATCH, D), 1.0, 6.0, ((1, 4), (2, 4)))
    weights = centred(seeds[1], (SECTIONS, D, D), (4 * D) ** -0.5, 0.046875, ((0, 2), (2, 4)))
    cotangent = centred(seeds[2], (MICRO, BATCH, D), 1.0, 6.0, ((1, 4), (2, 4)))
    hist_act = jnp.clip(jnp.exp(math.log(12.0) - 1.7917595 * jax.random.uniform(seeds[3], (SECTIONS, HIST), jnp.float32) ** steps_of(seeds[3], (SECTIONS, HIST), ((0, 2),), -0.2, 0.2)), 2.0, 12.0)
    hist_weight = jnp.clip(jnp.exp(math.log(0.1) - 2.3025851 * jax.random.uniform(seeds[4], (SECTIONS, HIST), jnp.float32) ** steps_of(seeds[4], (SECTIONS, HIST), ((0, 2),), -0.2, 0.2)), 0.01, 0.1)
    hist_grad = jnp.clip(jnp.exp(math.log(12.0) - 1.7917595 * jax.random.uniform(seeds[5], (SECTIONS, HIST), jnp.float32) ** steps_of(seeds[5], (SECTIONS, HIST), ((0, 2),), -0.2, 0.2)), 2.0, 12.0)
    return {"acts_in": acts_in, "weights": weights, "cotangent": cotangent, "hist_act": hist_act, "hist_weight": hist_weight, "hist_grad": hist_grad}


def quantize(values, factor, limit_value):
    return jnp.clip(values.astype(jnp.float32) * factor, -limit_value, limit_value).astype(jnp.bfloat16)


def settle(values):
    return lax.optimization_barrier(values.astype(jnp.bfloat16)).astype(jnp.float32)


def roll_history(history, newest):
    return jnp.concatenate([newest[:, None], history[:, :-1]], axis=1)


def reference(acts_in, weights, cotangent, hist_act, hist_weight, hist_grad):
    section_count = weights.shape[0]
    full_width = weights.shape[1]
    block_width = full_width // N_TENSOR
    current = acts_in.reshape(-1, full_width)
    act_factors = []
    weight_factors = []
    quant_acts = []
    quant_weights = []
    outputs = []
    act_peaks = []
    weight_peaks = []
    for section_index in range(section_count):
        act_factor = 448.0 / jnp.max(hist_act[section_index])
        weight_factor = 448.0 / jnp.max(hist_weight[section_index])
        quant_weight = quantize(weights[section_index], weight_factor, 448.0)
        quant_act = quantize(current, act_factor, 448.0)
        act_peaks.append(jnp.max(jnp.abs(current.astype(jnp.float32))))
        weight_peaks.append(jnp.max(jnp.abs(weights[section_index].astype(jnp.float32))))
        mixed_terms = jnp.dot(quant_act, quant_weight, preferred_element_type=jnp.float32) * (1.0 / (act_factor * weight_factor))
        current = (current.astype(jnp.float32) + mixed_terms).astype(jnp.bfloat16)
        outputs.append(current.reshape(MICRO, -1, full_width))
        act_factors.append(act_factor)
        weight_factors.append(weight_factor)
        quant_acts.append(quant_act)
        quant_weights.append(quant_weight)
    gradient = (cotangent.reshape(-1, full_width).astype(jnp.float32) * current.astype(jnp.float32)).astype(jnp.bfloat16)
    grads_out = [None] * section_count
    weight_sums = [None] * section_count
    grad_peaks = [None] * section_count
    for section_index in reversed(range(section_count)):
        grad_factor = 57344.0 / jnp.max(hist_grad[section_index])
        grad_peaks[section_index] = jnp.max(jnp.abs(gradient.astype(jnp.float32)))
        quant_grad = quantize(gradient, grad_factor, 57344.0)
        backward_factor = 1.0 / (grad_factor * weight_factors[section_index])
        sum_total = jnp.zeros((gradient.shape[0], full_width), jnp.float32)
        for shard_part in range(N_TENSOR):
            column_span = slice(shard_part * block_width, (shard_part + 1) * block_width)
            product_term = jnp.dot(quant_grad[:, column_span], quant_weights[section_index][:, column_span].T, preferred_element_type=jnp.float32) * backward_factor
            sum_total = sum_total + settle(product_term)
        gradient = (gradient.astype(jnp.float32) + sum_total).astype(jnp.bfloat16)
        grads_out[section_index] = gradient.reshape(MICRO, -1, full_width)
        update_factor = 1.0 / (act_factors[section_index] * grad_factor)
        acts_split = quant_acts[section_index].reshape(MICRO, N_DP, ROWS, full_width)
        grads_split = quant_grad.reshape(MICRO, N_DP, ROWS, full_width)
        weight_sum = jnp.zeros((full_width, full_width), jnp.float32)
        for dp_rank in range(N_DP):
            left_rows = acts_split[:, dp_rank].reshape(-1, full_width)
            right_rows = grads_split[:, dp_rank].reshape(-1, full_width)
            weight_sum = weight_sum + settle(jnp.dot(left_rows.T, right_rows, preferred_element_type=jnp.float32) * update_factor)
        weight_sums[section_index] = weight_sum.astype(jnp.bfloat16)
    section_acts = jnp.stack(outputs)
    section_grads = jnp.stack(grads_out)
    weight_grad = jnp.stack(weight_sums)
    new_hist_act = roll_history(hist_act, jnp.stack(act_peaks))
    new_hist_weight = roll_history(hist_weight, jnp.stack(weight_peaks))
    new_hist_grad = roll_history(hist_grad, jnp.stack(grad_peaks))
    return (section_acts, section_grads, weight_grad, new_hist_act, new_hist_weight, new_hist_grad)
```

```python
import functools

import jax
import jax.numpy as jnp
from jax import lax
from jax.experimental import pallas as pl
from jax.experimental.pallas import tpu as pltpu
from jax.sharding import PartitionSpec as P

MESH = pl.DeviceIdType.MESH
PIECES = 2
WIDE = 512


def strides_below(index, count):
    low = (index & -index) if index else count
    step, found = low // 2, []
    while step:
        found.append(step)
        step //= 2
    return found


def kernel(S, N, T, NC, RC, F, FA,
           acts, weights, cot, hist_a, hist_w, hist_g,
           out_acts, out_grads, out_w, out_ha, out_hw, out_hg,
           w, xin, xg, xout, acc, gin, part, rs, gout, G, A, dw, dwb, pk, amax, gmax,
           w_sem, x_ss, x_rs, ag_ss, ag_rs, g_ss, g_rs, rd_ss, rd_rs,
           G_ss, G_rs, A_ss, A_rs, B_ss, B_rs, p_ss, p_rs, o_sem, ow_sem):
    s, d, t = lax.axis_index("pipe"), lax.axis_index("dp"), lax.axis_index("tensor")
    last = S - 1
    bf, f32 = jnp.bfloat16, jnp.float32
    half = RC // 2

    def remote(src, dst, ss, rsem, **where):
        return pltpu.make_async_remote_copy(
            src_ref=src, dst_ref=dst, send_sem=ss, recv_sem=rsem,
            device_id=where, device_id_type=MESH)

    loads = [pltpu.make_async_copy(weights.at[b], w.at[b], w_sem.at[b]) for b in range(T)]
    for copy in loads:
        copy.start()

    barrier = pltpu.get_barrier_semaphore()
    for k in range(N):
        for j in range(T):
            if k or j:
                pl.semaphore_signal(barrier, inc=1, device_id={"dp": d ^ k, "tensor": t ^ j},
                                    device_id_type=MESH)

    @pl.when(s > 0)
    def _():
        pl.semaphore_signal(barrier, inc=1, device_id={"pipe": s - 1}, device_id_type=MESH)

    @pl.when(s < last)
    def _():
        pl.semaphore_signal(barrier, inc=1, device_id={"pipe": s + 1}, device_id_type=MESH)

    lim_a = jnp.max(hist_a[...], axis=1, keepdims=True).astype(bf)
    lim_w = jnp.max(hist_w[...], axis=1, keepdims=True).astype(bf)
    lim_g = jnp.max(hist_g[...], axis=1, keepdims=True).astype(bf)

    def clip(v, lim):
        return jnp.minimum(jnp.maximum(v, -lim), lim)

    def fold(v):
        return jnp.max(jnp.abs(v).reshape(-1, 16, v.shape[-1]), axis=0)

    amax[...] = jnp.zeros_like(amax)
    gmax[...] = jnp.zeros_like(gmax)

    near = (s > 0).astype(jnp.int32) + (s < last).astype(jnp.int32)
    pl.semaphore_wait(barrier, N * T - 1 + near)

    up = jnp.minimum(s + 1, last)
    down = jnp.maximum(s - 1, 0)

    def x_copy(c):
        return remote(xout.at[c], xin.at[c], x_ss.at[c], x_rs.at[c], pipe=up)

    def g_copy(c):
        return remote(gout.at[c], gin.at[c], g_ss.at[c], g_rs.at[c], pipe=down)

    def ag_copy(c, j, st):
        i = j ^ st
        return remote(xg.at[c, j], xg.at[c, i], ag_ss.at[c, i], ag_rs.at[c, i], tensor=t ^ st)

    def low(i):
        return i & -i

    def G_copy(c, j, st):
        i = j ^ st
        return remote(G.at[c, j], G.at[c, i], G_ss.at[c, i], G_rs.at[c, i], dp=d ^ st)

    ratio = N // T

    def in_block(r):
        start = lax.rem(r, ratio) * FA
        return t ^ lax.div(r, ratio), pl.ds(pl.multiple_of(start, FA), FA)

    def A_copy(c, k):
        rows = pl.ds(pl.multiple_of((t & 1) * half, half), half)
        owner, cols = in_block(d ^ k)
        return remote(xg.at[c, owner, rows, cols], A.at[c, k, rows], A_ss.at[c, k], A_rs.at[c, k],
                      dp=d ^ k)

    def B_copy(c, k):
        rows = pl.ds(pl.multiple_of((t & 1) * half, half), half)
        return remote(A.at[c, k, rows], A.at[c, k, rows], B_ss.at[c, k], B_rs.at[c, k],
                      tensor=t ^ 1)

    stages = []
    st = 1
    while st < T:
        stages.append(st)
        st *= 2

    def rd_copy(c, j, level):
        st = stages[level]
        i = j ^ st
        return remote(part.at[c, j], rs.at[c, level, i], rd_ss.at[c, j], rd_rs.at[c, level, i],
                      tensor=t ^ st)

    def prep(c):
        @pl.when(s == 0)
        def _():
            xin[c] = acts[c]

        @pl.when(s > 0)
        def _():
            x_copy(c).wait_recv()

        x = xin[c]
        xg[c, 0] = clip(x, lim_a)
        for st in strides_below(0, T):
            ag_copy(c, 0, st).start()
        amax[...] = jnp.maximum(amax[...], fold(x))

    def clip_weights():
        peak = jnp.zeros((16, F), bf)
        for b in range(T):
            loads[b].wait()

            def body(i, m, b=b):
                rows = pl.ds(pl.multiple_of(i * 128, 128), 128)
                v = w[b, rows]
                w[b, rows] = clip(v, lim_w)
                return jnp.maximum(m, fold(v))

            peak = lax.fori_loop(0, F // 128, body, peak)
        return jnp.max(peak.astype(f32), keepdims=True).reshape(1, 1)

    def compute(c):
        for j in range(T):
            if j:
                ag_copy(c, j ^ low(j), low(j)).wait_recv()
                for st in strides_below(j, T):
                    ag_copy(c, j, st).start()
            b = t ^ j

            def body(n, _, j=j, b=b):
                cols = pl.ds(pl.multiple_of(n * WIDE, WIDE), WIDE)
                y = jnp.dot(xg[c, j], w[b, :, cols], preferred_element_type=f32)
                if j == 0:
                    acc[:, cols] = y
                elif j < T - 1:
                    acc[:, cols] += y
                else:
                    xout[c, :, cols] = (acc[:, cols] + y + xin[c, :, cols].astype(f32)).astype(bf)
                return 0

            lax.fori_loop(0, F // WIDE, body, 0)

        @pl.when(s < last)
        def _():
            x_copy(c).start()

        pltpu.make_async_copy(xout.at[c], out_acts.at[c], o_sem.at[0, c]).start()
        for k in range(1, N):
            A_copy(c, k).start()
        owner, cols = in_block(d)
        A[c, 0] = xg[c, owner, :, cols]

    def prepb(c, is_last):
        if is_last:
            gin[c] = (cot[c].astype(f32) * xout[c].astype(f32)).astype(bf)
        else:
            g_copy(c).wait_recv()
        g = gin[c]
        G[c, 0] = clip(g, lim_g)
        for st in strides_below(0, N):
            G_copy(c, 0, st).start()
        gmax[...] = jnp.maximum(gmax[...], fold(g))
        order = sorted(range(T), key=lambda j: -(low(j) == 1))
        for j in order:
            b = t ^ j

            def body(n, _, j=j, b=b):
                cols = pl.ds(pl.multiple_of(n * WIDE, WIDE), WIDE)
                y = lax.dot_general(G[c, 0], w[b, cols, :], (((1,), (1,)), ((), ())),
                                    preferred_element_type=f32)
                part[c, j, :, cols] = y.astype(bf)
                return 0

            lax.fori_loop(0, F // WIDE, body, 0)
            if low(j) == 1:
                rd_copy(c, j, 0).start()

    def midb(c):
        for level in range(len(stages) - 1):
            st = stages[level]
            js = list(range(0, T, 2 * st))
            for j in sorted(js, key=lambda j: -(low(j) == 2 * st)):
                if j == 0:
                    continue
                rd_copy(c, j ^ st, level).wait_recv()
                part[c, j] = (part[c, j].astype(f32) + rs[c, level, j].astype(f32)).astype(bf)
                if low(j) == 2 * st:
                    rd_copy(c, j, level + 1).start()

    def finb(c):
        total = gin[c].astype(f32) + part[c, 0].astype(f32)
        for level in range(len(stages)):
            rd_copy(c, stages[level], level).wait_recv()
            total = total + rs[c, level, 0].astype(f32)
        gout[c] = total.astype(bf)

        @pl.when(s > 0)
        def _():
            g_copy(c).start()

        pltpu.make_async_copy(gout.at[c], out_grads.at[c], o_sem.at[1, c]).start()

    def relay_G(c):
        for j in range(1, N):
            G_copy(c, j ^ low(j), low(j)).wait_recv()
            for st in strides_below(j, N):
                G_copy(c, j, st).start()

    def relay_A(c):
        for k in range(1, N):
            A_copy(c, k).wait_recv()
            B_copy(c, k).start()

    def peers():
        return [(k, j) for k in range(N) for j in range(T) if k or j]

    def p_copy(k, j):
        i = k * T + j
        return remote(pk.at[0], pk.at[i], p_ss.at[i], p_rs.at[i], dp=d ^ k, tensor=t ^ j)

    def send_peaks():
        row = lax.broadcasted_iota(jnp.int32, (8, 128), 0)
        top_a = jnp.max(amax[...].astype(f32), keepdims=True).reshape(1, 1)
        top_g = jnp.max(gmax[...].astype(f32), keepdims=True).reshape(1, 1)
        pk[0] = jnp.where(row == 0, top_a, jnp.where(row == 1, w_peak, top_g))
        for k, j in peers():
            p_copy(k, j).start()

    prep(0)
    if NC > 1:
        prep(1)
    w_peak = clip_weights()

    def backward(i, is_last):
        if i < NC:
            prepb(i, is_last)
            if i == NC - 1:
                send_peaks()
            midb(i)
        if 1 <= i <= NC:
            finb(i - 1)

    @pl.when(s == last)
    def _():
        for c in range(NC):
            compute(c)
            if c + 2 < NC:
                prep(c + 2)
            if c >= 1:
                backward(c - 1, True)
        backward(NC - 1, True)
        backward(NC, True)
        for c in range(NC):
            relay_A(c)
            relay_G(c)

    @pl.when(s < last)
    def _():
        for c in range(NC):
            compute(c)
            if c + 2 < NC:
                prep(c + 2)
        for c in range(NC):
            relay_A(c)
        for c in range(NC + 1):
            backward(c, False)
            if c >= 1:
                relay_G(c - 1)

    for c in range(NC):
        for k in range(1, N):
            B_copy(c, k).wait_recv()
        tile = 256

        def body(n, _, c=c):
            cols = pl.ds(pl.multiple_of(n * tile, tile), tile)
            y = lax.dot_general(A[c, :, :, cols].reshape(N * RC, tile), G[c].reshape(N * RC, F),
                                (((0,), (0,)), ((), ())), preferred_element_type=f32)
            if c == 0:
                dw[cols, :] = y
            elif c < NC - 1:
                dw[cols, :] += y
            else:
                dwb[cols, :] = (dw[cols, :] + y).astype(bf)
            return 0

        lax.fori_loop(0, FA // tile, body, 0)
    out = pltpu.make_async_copy(dwb, out_w, ow_sem)
    out.start()

    for k, j in peers():
        p_copy(k, j).wait_recv()
    top = jnp.max(pk[...], axis=0)
    for row, (hist, out_hist) in enumerate(((hist_a, out_ha), (hist_w, out_hw), (hist_g, out_hg))):
        old = hist[...]
        out_hist[...] = jnp.concatenate([top[row:row + 1, 0:1], old[:, :-1]], axis=1)

    for c in range(NC):
        for i in range(1, T):
            ag_copy(c, i ^ low(i), low(i)).wait_send()
        for level, st in enumerate(stages):
            for j in range(0, T, st):
                if j & st:
                    rd_copy(c, j, level).wait_send()
        for i in range(1, N):
            G_copy(c, i ^ low(i), low(i)).wait_send()
            A_copy(c, i).wait_send()
            B_copy(c, i).wait_send()
        pltpu.make_async_copy(xout.at[c], out_acts.at[c], o_sem.at[0, c]).wait()
        pltpu.make_async_copy(gout.at[c], out_grads.at[c], o_sem.at[1, c]).wait()

        @pl.when(s < last)
        def _():
            x_copy(c).wait_send()

        @pl.when(s > 0)
        def _():
            g_copy(c).wait_send()

    for k, j in peers():
        p_copy(k, j).wait_send()
    out.wait()


def shards(acts_in, weights, cotangent, hist_act, hist_weight, hist_grad):
    S, N, T = lax.axis_size("pipe"), lax.axis_size("dp"), lax.axis_size("tensor")
    M, R, F = acts_in.shape
    NC, RC = M * PIECES, R // PIECES
    FA = T * F // N
    bf, f32 = jnp.bfloat16, jnp.float32
    levels = max(1, T.bit_length() - 1)
    dma = pltpu.SemaphoreType.DMA
    vmem = pl.BlockSpec(memory_space=pltpu.VMEM)
    anyw = pl.BlockSpec(memory_space=pl.ANY)
    hist = jax.ShapeDtypeStruct(hist_act.shape, f32)
    chunk = (NC, RC, F)
    result = pl.pallas_call(
        functools.partial(kernel, S, N, T, NC, RC, F, FA),
        out_shape=(jax.ShapeDtypeStruct(chunk, bf), jax.ShapeDtypeStruct(chunk, bf),
                   jax.ShapeDtypeStruct((FA, F), bf), hist, hist, hist),
        in_specs=[vmem, anyw, vmem, vmem, vmem, vmem],
        out_specs=(anyw, anyw, anyw, vmem, vmem, vmem),
        scratch_shapes=[
            pltpu.VMEM((T, F, F), bf),
            pltpu.VMEM(chunk, bf),
            pltpu.VMEM((NC, T, RC, F), bf),
            pltpu.VMEM(chunk, bf),
            pltpu.VMEM((RC, F), f32),
            pltpu.VMEM(chunk, bf),
            pltpu.VMEM((NC, T, RC, F), bf),
            pltpu.VMEM((NC, levels, T, RC, F), bf),
            pltpu.VMEM(chunk, bf),
            pltpu.VMEM((NC, N, RC, F), bf),
            pltpu.VMEM((NC, N, RC, FA), bf),
            pltpu.VMEM((FA, F), f32),
            pltpu.VMEM((FA, F), bf),
            pltpu.VMEM((N * T, 8, 128), f32),
            pltpu.VMEM((16, F), bf),
            pltpu.VMEM((16, F), bf),
            dma((T,)), dma((NC,)), dma((NC,)), dma((NC, T)), dma((NC, T)),
            dma((NC,)), dma((NC,)), dma((NC, T)), dma((NC, levels, T)),
            dma((NC, N)), dma((NC, N)), dma((NC, N)), dma((NC, N)), dma((NC, N)), dma((NC, N)),
            dma((N * T,)), dma((N * T,)), dma((2, NC)), dma(()),
        ],
        compiler_params=pltpu.CompilerParams(
            collective_id=0, has_side_effects=True, vmem_limit_bytes=60 * 2**20),
    )(acts_in.reshape(chunk), weights.reshape(T, F, F), cotangent.reshape(chunk),
      hist_act, hist_weight, hist_grad)
    out_acts, out_grads, out_w, ha, hw, hg = result
    return (out_acts.reshape(1, M, R, F), out_grads.reshape(1, M, R, F), out_w[None], ha, hw, hg)


def solution(mesh):
    placed = (P(None, "dp", "tensor"), P("pipe", None, "tensor"), P(None, "dp", "tensor"),
              P("pipe", None), P("pipe", None), P("pipe", None))
    return jax.shard_map(
        shards, mesh=mesh, in_specs=placed,
        out_specs=(P("pipe", None, "dp", "tensor"), P("pipe", None, "dp", "tensor"),
                   P("pipe", "dp", "tensor"), P("pipe", None), P("pipe", None), P("pipe", None)),
        check_vma=False)
```

```python
import functools

import jax
import jax.numpy as jnp
from jax import lax
from jax.experimental import pallas as pl
from jax.experimental.pallas import tpu as pltpu
from jax.sharding import PartitionSpec as P

MESH = pl.DeviceIdType.MESH
PIECES = 2
WIDE = 512


def strides_below(index, count):
    low = (index & -index) if index else count
    step, found = low // 2, []
    while step:
        found.append(step)
        step //= 2
    return found


def kernel(S, N, T, NC, RC, F, FA,
           acts, weights, cot, hist_a, hist_w, hist_g,
           out_acts, out_grads, out_w, out_ha, out_hw, out_hg,
           w, xin, xg, xout, acc, gin, part, rs, gout, G, A, dw, dwb, pk, amax, gmax,
           w_sem, x_ss, x_rs, ag_ss, ag_rs, g_ss, g_rs, rd_ss, rd_rs,
           G_ss, G_rs, A_ss, A_rs, B_ss, B_rs, p_ss, p_rs, o_sem, ow_sem):
    s, d, t = lax.axis_index("pipe"), lax.axis_index("dp"), lax.axis_index("tensor")
    last = S - 1
    bf, f32 = jnp.bfloat16, jnp.float32

    def remote(src, dst, ss, rsem, **where):
        return pltpu.make_async_remote_copy(
            src_ref=src, dst_ref=dst, send_sem=ss, recv_sem=rsem,
            device_id=where, device_id_type=MESH)

    loads = [pltpu.make_async_copy(weights.at[b], w.at[b], w_sem.at[b]) for b in range(T)]
    for copy in loads:
        copy.start()

    barrier = pltpu.get_barrier_semaphore()
    for k in range(N):
        for j in range(T):
            if k or j:
                pl.semaphore_signal(barrier, inc=1, device_id={"dp": d ^ k, "tensor": t ^ j},
                                    device_id_type=MESH)

    @pl.when(s > 0)
    def _():
        pl.semaphore_signal(barrier, inc=1, device_id={"pipe": s - 1}, device_id_type=MESH)

    @pl.when(s < last)
    def _():
        pl.semaphore_signal(barrier, inc=1, device_id={"pipe": s + 1}, device_id_type=MESH)

    lim_a = jnp.max(hist_a[...], axis=1, keepdims=True).astype(bf)
    lim_w = jnp.max(hist_w[...], axis=1, keepdims=True).astype(bf)
    lim_g = jnp.max(hist_g[...], axis=1, keepdims=True).astype(bf)

    def clip(v, lim):
        return jnp.minimum(jnp.maximum(v, -lim), lim)

    def fold(v):
        return jnp.max(jnp.abs(v).reshape(-1, 16, v.shape[-1]), axis=0)

    amax[...] = jnp.zeros_like(amax)
    gmax[...] = jnp.zeros_like(gmax)

    near = (s > 0).astype(jnp.int32) + (s < last).astype(jnp.int32)
    pl.semaphore_wait(barrier, N * T - 1 + near)

    up = jnp.minimum(s + 1, last)
    down = jnp.maximum(s - 1, 0)

    def x_copy(c):
        return remote(xout.at[c], xin.at[c], x_ss.at[c], x_rs.at[c], pipe=up)

    def g_copy(c):
        return remote(gout.at[c], gin.at[c], g_ss.at[c], g_rs.at[c], pipe=down)

    def ag_copy(c, j, st):
        i = j ^ st
        return remote(xg.at[c, j], xg.at[c, i], ag_ss.at[c, i], ag_rs.at[c, i], tensor=t ^ st)

    def low(i):
        return i & -i

    def G_copy(c, j, st):
        i = j ^ st
        return remote(G.at[c, j], G.at[c, i], G_ss.at[c, i], G_rs.at[c, i], dp=d ^ st)

    ratio = N // T

    def in_block(r):
        start = lax.rem(r, ratio) * FA
        return t ^ lax.div(r, ratio), pl.ds(pl.multiple_of(start, FA), FA)

    piece = RC // T

    def rows_of(owner):
        return pl.ds(pl.multiple_of(owner * piece, piece), piece)

    def A_copy(c, k):
        owner, cols = in_block(d ^ k)
        return remote(xg.at[c, owner, rows_of(t), cols], A.at[c, k, rows_of(t)],
                      A_ss.at[c, k], A_rs.at[c, k], dp=d ^ k)

    def B_copy(c, j, st):
        i = j ^ st
        there = A.at[c, pl.ds(1, N - 1), rows_of(t ^ j)]
        return remote(there, there, B_ss.at[c, i], B_rs.at[c, i], tensor=t ^ st)

    def B_arrival(c, i):
        there = A.at[c, pl.ds(1, N - 1), rows_of(t ^ i)]
        return remote(there, there, B_ss.at[c, i], B_rs.at[c, i], tensor=t ^ low(i))

    stages = []
    st = 1
    while st < T:
        stages.append(st)
        st *= 2

    def rd_copy(c, j, level):
        st = stages[level]
        i = j ^ st
        return remote(part.at[c, j], rs.at[c, level, i], rd_ss.at[c, j], rd_rs.at[c, level, i],
                      tensor=t ^ st)

    def prep(c):
        @pl.when(s == 0)
        def _():
            xin[c] = acts[c]

        @pl.when(s > 0)
        def _():
            x_copy(c).wait_recv()

        x = xin[c]
        xg[c, 0] = clip(x, lim_a)
        for st in strides_below(0, T):
            ag_copy(c, 0, st).start()
        amax[...] = jnp.maximum(amax[...], fold(x))

    def clip_weights():
        peak = jnp.zeros((16, F), bf)
        for b in range(T):
            loads[b].wait()

            def body(i, m, b=b):
                rows = pl.ds(pl.multiple_of(i * 128, 128), 128)
                v = w[b, rows]
                w[b, rows] = clip(v, lim_w)
                return jnp.maximum(m, fold(v))

            peak = lax.fori_loop(0, F // 128, body, peak)
        return jnp.max(peak.astype(f32), keepdims=True).reshape(1, 1)

    def compute(c):
        for j in range(T):
            if j:
                ag_copy(c, j ^ low(j), low(j)).wait_recv()
                for st in strides_below(j, T):
                    ag_copy(c, j, st).start()
            b = t ^ j

            def body(n, _, j=j, b=b):
                cols = pl.ds(pl.multiple_of(n * WIDE, WIDE), WIDE)
                y = jnp.dot(xg[c, j], w[b, :, cols], preferred_element_type=f32)
                if j == 0:
                    acc[:, cols] = y
                elif j < T - 1:
                    acc[:, cols] += y
                else:
                    xout[c, :, cols] = (acc[:, cols] + y + xin[c, :, cols].astype(f32)).astype(bf)
                return 0

            lax.fori_loop(0, F // WIDE, body, 0)

        @pl.when(s < last)
        def _():
            x_copy(c).start()

        pltpu.make_async_copy(xout.at[c], out_acts.at[c], o_sem.at[0, c]).start()
        for k in range(1, N):
            A_copy(c, k).start()
        owner, cols = in_block(d)
        A[c, 0] = xg[c, owner, :, cols]

    def prepb(c, is_last):
        if is_last:
            gin[c] = (cot[c].astype(f32) * xout[c].astype(f32)).astype(bf)
        else:
            g_copy(c).wait_recv()
        g = gin[c]
        G[c, 0] = clip(g, lim_g)
        for st in strides_below(0, N):
            G_copy(c, 0, st).start()
        gmax[...] = jnp.maximum(gmax[...], fold(g))
        order = sorted(range(T), key=lambda j: -(low(j) == 1))
        for j in order:
            b = t ^ j

            def body(n, _, j=j, b=b):
                cols = pl.ds(pl.multiple_of(n * WIDE, WIDE), WIDE)
                y = lax.dot_general(G[c, 0], w[b, cols, :], (((1,), (1,)), ((), ())),
                                    preferred_element_type=f32)
                part[c, j, :, cols] = y.astype(bf)
                return 0

            lax.fori_loop(0, F // WIDE, body, 0)
            if low(j) == 1:
                rd_copy(c, j, 0).start()

    def midb(c):
        for level in range(len(stages) - 1):
            st = stages[level]
            js = list(range(0, T, 2 * st))
            for j in sorted(js, key=lambda j: -(low(j) == 2 * st)):
                if j == 0:
                    continue
                rd_copy(c, j ^ st, level).wait_recv()
                part[c, j] = (part[c, j].astype(f32) + rs[c, level, j].astype(f32)).astype(bf)
                if low(j) == 2 * st:
                    rd_copy(c, j, level + 1).start()

    def finb(c):
        total = gin[c].astype(f32) + part[c, 0].astype(f32)
        for level in range(len(stages)):
            rd_copy(c, stages[level], level).wait_recv()
            total = total + rs[c, level, 0].astype(f32)
        gout[c] = total.astype(bf)

        @pl.when(s > 0)
        def _():
            g_copy(c).start()

        pltpu.make_async_copy(gout.at[c], out_grads.at[c], o_sem.at[1, c]).start()

    def relay_G(c):
        for j in range(1, N):
            if strides_below(j, N):
                G_copy(c, j ^ low(j), low(j)).wait_recv()
                for st in strides_below(j, N):
                    G_copy(c, j, st).start()

    def relay_A(c):
        for k in range(1, N):
            A_copy(c, k).wait_recv()
        for st in strides_below(0, T):
            B_copy(c, 0, st).start()

    def relay_B(c):
        for j in range(1, T):
            if strides_below(j, T):
                B_arrival(c, j).wait_recv()
                for st in strides_below(j, T):
                    B_copy(c, j, st).start()

    def update(c):
        for j in range(1, N):
            if not strides_below(j, N):
                G_copy(c, j ^ low(j), low(j)).wait_recv()
        for j in range(1, T):
            if not strides_below(j, T):
                B_arrival(c, j).wait_recv()
        tile = 256

        def body(n, _):
            cols = pl.ds(pl.multiple_of(n * tile, tile), tile)
            y = lax.dot_general(A[c, :, :, cols].reshape(N * RC, tile), G[c].reshape(N * RC, F),
                                (((0,), (0,)), ((), ())), preferred_element_type=f32)
            if c == 0:
                dw[cols, :] = y
            elif c < NC - 1:
                dw[cols, :] += y
            else:
                dwb[cols, :] = (dw[cols, :] + y).astype(bf)
            return 0

        lax.fori_loop(0, FA // tile, body, 0)

    def peers():
        return [(k, j) for k in range(N) for j in range(T) if k or j]

    def p_copy(k, j):
        i = k * T + j
        return remote(pk.at[0], pk.at[i], p_ss.at[i], p_rs.at[i], dp=d ^ k, tensor=t ^ j)

    def send_peaks():
        row = lax.broadcasted_iota(jnp.int32, (8, 128), 0)
        top_a = jnp.max(amax[...].astype(f32), keepdims=True).reshape(1, 1)
        top_g = jnp.max(gmax[...].astype(f32), keepdims=True).reshape(1, 1)
        pk[0] = jnp.where(row == 0, top_a, jnp.where(row == 1, w_peak, top_g))
        for k, j in peers():
            p_copy(k, j).start()

    prep(0)
    if NC > 1:
        prep(1)
    w_peak = clip_weights()

    def backward(i, is_last):
        if i < NC:
            prepb(i, is_last)
            if i == NC - 1:
                send_peaks()
            midb(i)
        if 1 <= i <= NC:
            finb(i - 1)

    @pl.when(s == last)
    def _():
        for c in range(NC):
            compute(c)
            if c + 2 < NC:
                prep(c + 2)
            if c >= 1:
                backward(c - 1, True)
        backward(NC - 1, True)
        backward(NC, True)
        for c in range(NC):
            relay_A(c)
            relay_G(c)
        for c in range(NC):
            relay_B(c)
        for c in range(NC - 1):
            update(c)

    @pl.when(s < last)
    def _():
        for c in range(NC):
            compute(c)
            if c + 2 < NC:
                prep(c + 2)
        for c in range(NC):
            relay_A(c)
        for c in range(NC):
            relay_B(c)
        for c in range(NC + 1):
            backward(c, False)
            if c >= 1:
                relay_G(c - 1)
            if c >= 3:
                update(c - 3)
        for c in range(NC - 2, NC - 1):
            update(c)

    update(NC - 1)
    out = pltpu.make_async_copy(dwb, out_w, ow_sem)
    out.start()

    for k, j in peers():
        p_copy(k, j).wait_recv()
    top = jnp.max(pk[...], axis=0)
    for row, (hist, out_hist) in enumerate(((hist_a, out_ha), (hist_w, out_hw), (hist_g, out_hg))):
        old = hist[...]
        out_hist[...] = jnp.concatenate([top[row:row + 1, 0:1], old[:, :-1]], axis=1)

    for c in range(NC):
        for i in range(1, T):
            ag_copy(c, i ^ low(i), low(i)).wait_send()
        for level, st in enumerate(stages):
            for j in range(0, T, st):
                if j & st:
                    rd_copy(c, j, level).wait_send()
        for i in range(1, N):
            G_copy(c, i ^ low(i), low(i)).wait_send()
            A_copy(c, i).wait_send()
        for i in range(1, T):
            B_copy(c, i ^ low(i), low(i)).wait_send()
        pltpu.make_async_copy(xout.at[c], out_acts.at[c], o_sem.at[0, c]).wait()
        pltpu.make_async_copy(gout.at[c], out_grads.at[c], o_sem.at[1, c]).wait()

        @pl.when(s < last)
        def _():
            x_copy(c).wait_send()

        @pl.when(s > 0)
        def _():
            g_copy(c).wait_send()

    for k, j in peers():
        p_copy(k, j).wait_send()
    out.wait()


def shards(acts_in, weights, cotangent, hist_act, hist_weight, hist_grad):
    S, N, T = lax.axis_size("pipe"), lax.axis_size("dp"), lax.axis_size("tensor")
    M, R, F = acts_in.shape
    NC, RC = M * PIECES, R // PIECES
    FA = T * F // N
    bf, f32 = jnp.bfloat16, jnp.float32
    levels = max(1, T.bit_length() - 1)
    dma = pltpu.SemaphoreType.DMA
    vmem = pl.BlockSpec(memory_space=pltpu.VMEM)
    anyw = pl.BlockSpec(memory_space=pl.ANY)
    hist = jax.ShapeDtypeStruct(hist_act.shape, f32)
    chunk = (NC, RC, F)
    result = pl.pallas_call(
        functools.partial(kernel, S, N, T, NC, RC, F, FA),
        out_shape=(jax.ShapeDtypeStruct(chunk, bf), jax.ShapeDtypeStruct(chunk, bf),
                   jax.ShapeDtypeStruct((FA, F), bf), hist, hist, hist),
        in_specs=[vmem, anyw, vmem, vmem, vmem, vmem],
        out_specs=(anyw, anyw, anyw, vmem, vmem, vmem),
        scratch_shapes=[
            pltpu.VMEM((T, F, F), bf),
            pltpu.VMEM(chunk, bf),
            pltpu.VMEM((NC, T, RC, F), bf),
            pltpu.VMEM(chunk, bf),
            pltpu.VMEM((RC, F), f32),
            pltpu.VMEM(chunk, bf),
            pltpu.VMEM((NC, T, RC, F), bf),
            pltpu.VMEM((NC, levels, T, RC, F), bf),
            pltpu.VMEM(chunk, bf),
            pltpu.VMEM((NC, N, RC, F), bf),
            pltpu.VMEM((NC, N, RC, FA), bf),
            pltpu.VMEM((FA, F), f32),
            pltpu.VMEM((FA, F), bf),
            pltpu.VMEM((N * T, 8, 128), f32),
            pltpu.VMEM((16, F), bf),
            pltpu.VMEM((16, F), bf),
            dma((T,)), dma((NC,)), dma((NC,)), dma((NC, T)), dma((NC, T)),
            dma((NC,)), dma((NC,)), dma((NC, T)), dma((NC, levels, T)),
            dma((NC, N)), dma((NC, N)), dma((NC, N)), dma((NC, N)), dma((NC, T)), dma((NC, T)),
            dma((N * T,)), dma((N * T,)), dma((2, NC)), dma(()),
        ],
        compiler_params=pltpu.CompilerParams(
            collective_id=0, has_side_effects=True, vmem_limit_bytes=60 * 2**20),
    )(acts_in.reshape(chunk), weights.reshape(T, F, F), cotangent.reshape(chunk),
      hist_act, hist_weight, hist_grad)
    out_acts, out_grads, out_w, ha, hw, hg = result
    return (out_acts.reshape(1, M, R, F), out_grads.reshape(1, M, R, F), out_w[None], ha, hw, hg)


def solution(mesh):
    placed = (P(None, "dp", "tensor"), P("pipe", None, "tensor"), P(None, "dp", "tensor"),
              P("pipe", None), P("pipe", None), P("pipe", None))
    return jax.shard_map(
        shards, mesh=mesh, in_specs=placed,
        out_specs=(P("pipe", None, "dp", "tensor"), P("pipe", None, "dp", "tensor"),
                   P("pipe", "dp", "tensor"), P("pipe", None), P("pipe", None), P("pipe", None)),
        check_vma=False)
```
